32 devices in a mesh: cpi: 2 (over y), rng: 4 (over z), bin: 2 (over x), chn: 2 (over core).
Axes of the slice: x: 2, y: 2, z: 4, core: 2. Of those that a mesh axis runs over, the one named last changes fastest.
Arguments:
- samples: bfloat16 [16, 8192, 384], P(('cpi', 'bin'), 'rng', 'chn'), parts along dimension 0, may hold values from -16 to 16
- train_mask: int32 [16, 8192], P(('cpi', 'bin'), 'rng'), parts along dimension 0, may hold values 0 or 1
- angles: int32 [32], P('cpi'), parts along dimension 0, may hold values from 0 to 127
Outputs:
- amf_stat: float32 [16, 16, 8192], P(('cpi', 'bin'), None, ('rng', 'chn')), parts along dimension 0
- gate_power: float32 [16, 8192], P(('cpi', 'bin'), ('rng', 'chn')), parts along dimension 0
The draws below stay inside these ranges and needn't reach their ends.
There are 2 independent parts, one for each index of `cpi`. The reference program is written for one: setup_inputs(seed, part) draws one part's arguments, and reference() takes and returns one part's arrays. A program takes and returns all parts, laid end to end along the dimension named above; each array names one. Nothing has to cross between parts.
All inputs are finite; a program needn't handle non-finite values. No bound on the sum of `train_mask` on one device may be relied on, other than what follows from the above.
Results may differ from the reference program's by a relative error of at most 0.0004.
Values may be sent and summed in bfloat16 or wider, within the bound.
A program may use at most 128 MiB of HBM per device.

```python
import jax
import jax.numpy as jnp
from jax import lax

C = 384
NS = 16
ANGLES = 128
NB = 8
GATES = 8192


def draw_samples(key, part):
    keys = jax.random.split(jax.random.fold_in(key, 11), 4)
    base = jax.random.normal(keys[0], (NB, GATES, C), jnp.float32)
    mixing = jnp.eye(C, dtype=jnp.float32)[None] + 0.5 * jax.random.normal(keys[1], (NB, C, C), jnp.float32) / jnp.sqrt(C * 1.0)
    mixed = jnp.einsum('bgc,bcd->bgd', base, mixing)
    offsets = jax.random.uniform(keys[2], (NB, 1), jnp.float32, 0.0, 6.283)
    gate_pos = jnp.arange(GATES).astype(jnp.float32)[None, :] / GATES
    profile = jnp.exp(0.5 * jax.random.normal(keys[3], (NB, GATES), jnp.float32) + 0.6 * jnp.cos(6.283 * 3.0 * gate_pos + offsets))
    result = mixed * profile[:, :, None]
    return jnp.clip(result, -16.0, 16.0).astype(jnp.bfloat16)


def with_ends(drawn, rng, least, largest):
    index_at = [jax.random.randint(jax.random.fold_in(rng, axis), (), 0, length) for axis, length in enumerate(drawn.shape)]
    longest = drawn.shape.index(max(drawn.shape))
    next_to = index_at[:longest] + [(index_at[longest] + 1) % drawn.shape[longest]] + index_at[longest + 1:]
    return drawn.at[tuple(index_at)].set(least).at[tuple(next_to)].set(largest)


def setup_inputs(seed: int = 0, part: int = 0) -> dict:
    streams_of = jax.random.split(jax.random.key(seed), 4)
    part_keys = jax.random.split(jax.random.fold_in(streams_of[3], part), 4)
    return {
        "samples": draw_samples(jax.random.fold_in(jax.random.fold_in(streams_of[3], part), 71), part),
        "train_mask": with_ends((jax.random.randint(part_keys[1], (NB, GATES), 0, 4) < 3).astype(jnp.int32), jax.random.fold_in(part_keys[1], 1), 0, 1),
        "angles": with_ends(jax.random.randint(part_keys[2], (NS,), 0, ANGLES), jax.random.fold_in(part_keys[2], 1), 0, ANGLES - 1).astype(jnp.int32),
    }


LOAD = 0.1

def steering(angles, channels):
    elements = channels // 2
    phase = jnp.pi * jnp.sin(jnp.pi * (angles.astype(jnp.float32) / ANGLES - 0.5))
    element_pos = jnp.arange(elements).astype(jnp.float32)
    turns = element_pos[:, None] * phase[None, :]
    return jnp.concatenate([jnp.cos(turns), jnp.sin(turns)], axis=0)

def reference(samples, train_mask, angles):
    steer = steering(angles, C)
    identity = jnp.eye(C, dtype=jnp.float32)

    def one_bin(block):
        block_samples, block_mask = block
        weights = block_mask.astype(jnp.bfloat16)
        masked = block_samples * weights[:, None]
        gram_sum = jnp.dot(masked.T.astype(jnp.float32), block_samples.astype(jnp.float32), preferred_element_type=jnp.float32)
        counts = jnp.sum(block_mask.astype(jnp.float32))
        covariance = gram_sum / jnp.maximum(counts, 1.0) + LOAD * identity
        factor = jnp.linalg.cholesky(covariance)
        white_steer = jax.scipy.linalg.solve_triangular(factor, steer, lower=True)
        steer_power = jnp.sum(white_steer * white_steer, axis=0)
        filters = jax.scipy.linalg.solve_triangular(factor, white_steer, lower=True, trans=1)
        columns = block_samples.astype(jnp.float32).T
        projected = jnp.dot(filters.T, columns, precision=lax.Precision.HIGHEST)
        amf_stat = projected * projected / steer_power[:, None]
        white_gates = jax.scipy.linalg.solve_triangular(factor, columns, lower=True)
        gate_power = jnp.sum(white_gates * white_gates, axis=0) / C
        return (amf_stat, gate_power)
    amf_stat, gate_power = lax.map(one_bin, (samples, train_mask))
    return (amf_stat, gate_power)
```

```python
import functools

import jax
import jax.numpy as jnp
from jax import lax
from jax.experimental import pallas as pl
from jax.experimental.pallas import tpu as pltpu
from jax.sharding import PartitionSpec as P

ANGLES = 128
LOAD = 0.1
T = 128
MESH = pl.DeviceIdType.MESH
HIGH = lax.Precision.HIGHEST


def steering(angles, channels):
    elements = channels // 2
    phase = jnp.pi * jnp.sin(jnp.pi * (angles.astype(jnp.float32) / ANGLES - 0.5))
    element_pos = jnp.arange(elements).astype(jnp.float32)
    turns = element_pos[:, None] * phase[None, :]
    return jnp.concatenate([jnp.cos(turns), jnp.sin(turns)], axis=0)


def whiten_and_test(gram_sum, counts, tested, angles):
    channels = tested.shape[2]
    identity = jnp.eye(channels, dtype=jnp.float32)
    covariance = gram_sum / jnp.maximum(counts, 1.0)[:, None, None] + LOAD * identity[None]
    factor = jnp.linalg.cholesky(covariance)
    steer = steering(angles, channels)
    steer_batch = jnp.broadcast_to(steer, (factor.shape[0],) + steer.shape)
    white_steer = jax.scipy.linalg.solve_triangular(factor, steer_batch, lower=True)
    steer_power = jnp.sum(white_steer * white_steer, axis=1)
    filters = jax.scipy.linalg.solve_triangular(factor, white_steer, lower=True, trans=1)
    columns = jnp.swapaxes(tested.astype(jnp.float32), 1, 2)
    projected = jnp.einsum("bck,bcg->bkg", filters, columns, precision=lax.Precision.HIGHEST)
    amf_stat = projected * projected / steer_power[:, :, None]
    white_gates = jax.scipy.linalg.solve_triangular(factor, columns, lower=True)
    gate_power = jnp.sum(white_gates * white_gates, axis=1) / channels
    return (amf_stat, gate_power)


def plain_body(samples, train_mask, angles):
    cores = lax.axis_size("chn")
    core_index = lax.axis_index("chn")
    half_gates = samples.shape[1] // cores
    complete = lax.all_gather(samples, "chn", axis=2, tiled=True)
    weights = train_mask.astype(jnp.bfloat16)
    masked = samples * weights[:, :, None]
    row_part = jnp.einsum("bgc,bgd->bcd", masked, complete, preferred_element_type=jnp.float32)
    count_part = jnp.sum(train_mask.astype(jnp.float32), axis=1)
    row_sum, counts = lax.psum((row_part, count_part), "rng")
    gram_sum = lax.all_gather(row_sum, "chn", axis=1, tiled=True)
    tested = lax.dynamic_slice_in_dim(complete, core_index * half_gates, half_gates, 1)
    return whiten_and_test(gram_sum, counts, tested, angles)


def invert_tile(a):
    n = a.shape[0]
    sub = lax.broadcasted_iota(jnp.int32, (8, n), 0)
    lane = lax.broadcasted_iota(jnp.int32, (8, n), 1)
    lane_all = lax.broadcasted_iota(jnp.int32, (n, n), 1)
    for g in range(0, n, 8):
        slab = a[g:g + 8, :]
        cols = [jnp.broadcast_to(slab[:, g + j:g + j + 1], (8, n)) for j in range(8)]
        inside = (lane >= g) & (lane < g + 8)
        slab = jnp.where(inside, jnp.where(lane - g == sub, 1.0, 0.0), slab)
        for k in range(8):
            scale = 1.0 / cols[k][k:k + 1, :]
            row = slab[k:k + 1, :] * scale
            slab = jnp.where(sub == k, row, slab - cols[k] * row)
            for j in range(k + 1, 8):
                crow = cols[j][k:k + 1, :] * scale
                cols[j] = jnp.where(sub == k, crow, cols[j] - cols[k] * crow)
        rest = jnp.where((lane_all >= g) & (lane_all < g + 8), 0.0, a)
        for j in range(8):
            rest = rest - a[:, g + j:g + j + 1] * slab[j:j + 1, :]
        pieces = [slab]
        if g:
            pieces = [rest[:g, :]] + pieces
        if g + 8 < n:
            pieces = pieces + [rest[g + 8:, :]]
        a = jnp.concatenate(pieces, axis=0)
    return a


def dot(a, b, precision=None):
    return jnp.dot(a, b, precision=precision, preferred_element_type=jnp.float32)


def split3(a):
    hi = a.astype(jnp.bfloat16)
    left = a - hi.astype(jnp.float32)
    mid = left.astype(jnp.bfloat16)
    lo = (left - mid.astype(jnp.float32)).astype(jnp.bfloat16)
    return hi, mid, lo


def kernel(n, lower, x_hbm, mask_ref, steer_ref, amf_ref, pow_ref,
           own, got, xt, gram, gram_rx, part, rs_rx, red, red_rx, mat, inv, ag_rx, fwd_rx, full,
           lsem, xs, xr, gs, gr, rss, rsr, ds, dr, ags, agr, fs, fr):
    r = lax.axis_index("rng")
    c = lax.axis_index("chn")
    other = 1 - c
    bins, half, width = own.shape
    chans = 2 * width
    nb = chans // T
    share = len(lower) // 2
    rows = share * T

    barrier = pltpu.get_barrier_semaphore()
    pl.semaphore_signal(barrier, inc=1, device_id={"chn": other}, device_id_type=MESH)
    for d in range(1, n):
        pl.semaphore_signal(barrier, inc=1, device_id={"rng": lax.rem(r + d, n)}, device_id_type=MESH)

    order = [lax.rem(r + d, n) for d in range(1, n)] + [r]
    loads = []
    for i, b in enumerate(order):
        cp = pltpu.make_async_copy(x_hbm.at[b, pl.ds(pl.multiple_of(c * half, T), half), :], own.at[b], lsem.at[i])
        cp.start()
        loads.append(cp)
    pl.semaphore_wait(barrier, n)

    def remote(src, dst, send, recv, where):
        cp = pltpu.make_async_remote_copy(src_ref=src, dst_ref=dst, send_sem=send, recv_sem=recv,
                                          device_id=where, device_id_type=MESH)
        cp.start()
        return cp

    swaps = [remote(x_hbm.at[b, pl.ds(pl.multiple_of(other * half, T), half), :], got.at[b],
                    xs.at[i], xr.at[i], {"chn": other}) for i, b in enumerate(order)]

    sends = []

    def reduce_pair(i, b):
        swap = gsw[i]
        swap.wait()
        for s in range(share):
            part[b, s * T:(s + 1) * T, :] = gram[b, c * share + s] + gram_rx[b, s]
        count = jnp.sum(mask_ref[b].astype(jnp.float32))
        part[b, rows:rows + 8, :] = jnp.full((8, T), count, jnp.float32)
        if i < n - 1:
            sends.append(remote(part.at[b], rs_rx.at[i], rss.at[i], rsr.at[i], {"rng": b}))

    gsw = []
    for i, b in enumerate(order):
        loads[i].wait()
        swaps[i].wait()
        mine, theirs = own[b], got[b]
        first = c == 0
        xt[b, :width, :] = jnp.where(first, mine, theirs).T
        xt[b, width:, :] = jnp.where(first, theirs, mine).T
        mask = mask_ref[b, :, pl.ds(pl.multiple_of(c * half, T), half)].astype(jnp.bfloat16)
        xb = xt[b]
        g = lax.dot_general(xb * mask, xb, (((1,), (1,)), ((), ())), preferred_element_type=jnp.float32)
        for s, (p, q) in enumerate(lower):
            gram[b, s] = g[p * T:(p + 1) * T, q * T:(q + 1) * T]
        gsw.append(remote(gram.at[b, pl.ds(other * share, share)], gram_rx.at[b], gs.at[i], gr.at[i], {"chn": other}))
        if i:
            reduce_pair(i - 1, order[i - 1])
    reduce_pair(n - 1, r)

    total = part[r]
    for cp in sends:
        cp.wait()
    for d in range(n - 1):
        total = total + rs_rx[d]
    red[...] = total
    cp = remote(red, red_rx, ds, dr, {"chn": other})
    scale = jnp.maximum(total[rows:rows + 1, :], 1.0)
    cp.wait()
    diag = jnp.where(lax.broadcasted_iota(jnp.int32, (T, T), 0) == lax.broadcasted_iota(jnp.int32, (T, T), 1), LOAD, 0.0)
    for s, (p, q) in enumerate(lower):
        lo = (s % share) * T
        a, b = red[lo:lo + T, :], red_rx[lo:lo + T, :]
        block = jnp.where(c == s // share, a, b) / scale
        if p == q:
            mat[p, p] = block + diag
        else:
            mat[p, q] = block
            mat[q, p] = block.T

    @pl.loop(0, nb)
    def _(p):
        tile = invert_tile(mat[p, p])
        others = [lax.rem(p + d, nb) for d in range(1, nb)]
        cross = [dot(tile, mat[p, j], HIGH) for j in others]
        for i in others:
            col = mat[i, p]
            for j, e in zip(others, cross):
                mat[i, j] = mat[i, j] - dot(col, e, HIGH)
            mat[i, p] = -dot(col, tile, HIGH)
        mat[p, p] = tile
        for j, e in zip(others, cross):
            mat[p, j] = e

    for s, (p, q) in enumerate(lower):
        inv[s] = mat[p, q]
    gathers = [remote(inv.at[pl.ds(c * share, share)], ag_rx.at[d - 1], ags.at[d - 1], agr.at[d - 1],
                      {"rng": lax.rem(r + d, n)}) for d in range(1, n)]
    steer = steer_ref[...]
    k = steer.shape[0]

    def finish(b, blocks):
        for (p, q), block in zip(lower, blocks):
            full[p * T:(p + 1) * T, q * T:(q + 1) * T] = block
            if p != q:
                full[q * T:(q + 1) * T, p * T:(p + 1) * T] = block.T
        s = full[...]
        f = dot(steer, s, HIGH)
        power = jnp.sum(f * steer, axis=1, keepdims=True)
        xb = xt[b]
        y = sum(dot(m, xb) for m in split3(s))
        pow_ref[b] = jnp.sum(y * xb.astype(jnp.float32), axis=0, keepdims=True) / chans
        z = sum(dot(m, xb) for m in split3(f))
        amf_ref[b] = z * z / power

    finish(r, [inv[s] for s in range(len(lower))])
    forwards = []
    for d in range(1, n):
        gathers[d - 1].wait()
        forwards.append(remote(ag_rx.at[d - 1], fwd_rx.at[d - 1], fs.at[d - 1], fr.at[d - 1], {"chn": other}))
    for d in range(1, n):
        forwards[d - 1].wait()
        blocks = [jnp.where(c == s // share, ag_rx[d - 1, s % share], fwd_rx[d - 1, s % share])
                  for s in range(len(lower))]
        finish(lax.rem(r - d + n, n), blocks)


def fused_body(samples, train_mask, angles):
    bins, gates, width = samples.shape
    n = lax.axis_size("rng")
    half, chans = gates // 2, 2 * width
    nb = chans // T
    lower = [(i, j) for i in range(nb) for j in range(i + 1)]
    share = len(lower) // 2
    steer = steering(angles, chans).T
    f32, bf16 = jnp.float32, jnp.bfloat16
    sem = pltpu.SemaphoreType.DMA
    vmem = pl.BlockSpec(memory_space=pltpu.VMEM)
    rows = share * T + 8
    amf, power = pl.pallas_call(
        functools.partial(kernel, n, lower),
        name="amf",
        out_shape=(jax.ShapeDtypeStruct((bins, steer.shape[0], half), f32),
                   jax.ShapeDtypeStruct((bins, 1, half), f32)),
        in_specs=[pl.BlockSpec(memory_space=pl.ANY), vmem, vmem],
        out_specs=(vmem, vmem),
        scratch_shapes=[
            pltpu.VMEM((bins, half, width), bf16),
            pltpu.VMEM((bins, half, width), bf16),
            pltpu.VMEM((bins, chans, half), bf16),
            pltpu.VMEM((bins, len(lower), T, T), f32),
            pltpu.VMEM((bins, share, T, T), f32),
            pltpu.VMEM((bins, rows, T), f32),
            pltpu.VMEM((n - 1, rows, T), f32),
            pltpu.VMEM((rows, T), f32),
            pltpu.VMEM((rows, T), f32),
            pltpu.VMEM((nb, nb, T, T), f32),
            pltpu.VMEM((len(lower), T, T), f32),
            pltpu.VMEM((n - 1, share, T, T), f32),
            pltpu.VMEM((n - 1, share, T, T), f32),
            pltpu.VMEM((chans, chans), f32),
            sem((n,)), sem((n,)), sem((n,)), sem((n,)), sem((n,)),
            sem((n - 1,)), sem((n - 1,)), sem, sem,
            sem((n - 1,)), sem((n - 1,)), sem((n - 1,)), sem((n - 1,)),
        ],
        compiler_params=pltpu.CompilerParams(collective_id=0, has_side_effects=True, vmem_limit_bytes=56 * 2**20),
    )(samples, train_mask[:, None, :], steer)
    return amf, power[:, 0, :]


def solution(mesh):
    placed = (P(("cpi", "bin"), "rng", "chn"), P(("cpi", "bin"), "rng"), P("cpi"))

    def body(samples, train_mask, angles):
        bins, gates, width = samples.shape
        nb = 2 * width // T
        fits = (mesh.shape["chn"] == 2 and mesh.shape["rng"] == bins and bins > 1 and (2 * width) % T == 0
                and gates % (2 * T) == 0 and nb * (nb + 1) // 2 % 2 == 0)
        return (fused_body if fits else plain_body)(samples, train_mask, angles)

    return jax.shard_map(
        body,
        mesh=mesh,
        in_specs=placed,
        out_specs=(P(("cpi", "bin"), None, ("rng", "chn")), P(("cpi", "bin"), ("rng", "chn"))),
        check_vma=False,
    )
```

```python
import functools

import jax
import jax.numpy as jnp
from jax import lax
from jax.experimental import pallas as pl
from jax.experimental.pallas import tpu as pltpu
from jax.sharding import PartitionSpec as P

ANGLES = 128
LOAD = 0.1
T = 128
MESH = pl.DeviceIdType.MESH
HIGH = lax.Precision.HIGHEST


def steering(angles, channels):
    elements = channels // 2
    phase = jnp.pi * jnp.sin(jnp.pi * (angles.astype(jnp.float32) / ANGLES - 0.5))
    element_pos = jnp.arange(elements).astype(jnp.float32)
    turns = element_pos[:, None] * phase[None, :]
    return jnp.concatenate([jnp.cos(turns), jnp.sin(turns)], axis=0)


def whiten_and_test(gram_sum, counts, tested, angles):
    channels = tested.shape[2]
    identity = jnp.eye(channels, dtype=jnp.float32)
    covariance = gram_sum / jnp.maximum(counts, 1.0)[:, None, None] + LOAD * identity[None]
    factor = jnp.linalg.cholesky(covariance)
    steer = steering(angles, channels)
    steer_batch = jnp.broadcast_to(steer, (factor.shape[0],) + steer.shape)
    white_steer = jax.scipy.linalg.solve_triangular(factor, steer_batch, lower=True)
    steer_power = jnp.sum(white_steer * white_steer, axis=1)
    filters = jax.scipy.linalg.solve_triangular(factor, white_steer, lower=True, trans=1)
    columns = jnp.swapaxes(tested.astype(jnp.float32), 1, 2)
    projected = jnp.einsum("bck,bcg->bkg", filters, columns, precision=lax.Precision.HIGHEST)
    amf_stat = projected * projected / steer_power[:, :, None]
    white_gates = jax.scipy.linalg.solve_triangular(factor, columns, lower=True)
    gate_power = jnp.sum(white_gates * white_gates, axis=1) / channels
    return (amf_stat, gate_power)


def plain_body(samples, train_mask, angles):
    cores = lax.axis_size("chn")
    core_index = lax.axis_index("chn")
    half_gates = samples.shape[1] // cores
    complete = lax.all_gather(samples, "chn", axis=2, tiled=True)
    weights = train_mask.astype(jnp.bfloat16)
    masked = samples * weights[:, :, None]
    row_part = jnp.einsum("bgc,bgd->bcd", masked, complete, preferred_element_type=jnp.float32)
    count_part = jnp.sum(train_mask.astype(jnp.float32), axis=1)
    row_sum, counts = lax.psum((row_part, count_part), "rng")
    gram_sum = lax.all_gather(row_sum, "chn", axis=1, tiled=True)
    tested = lax.dynamic_slice_in_dim(complete, core_index * half_gates, half_gates, 1)
    return whiten_and_test(gram_sum, counts, tested, angles)


def invert_tile(a):
    n = a.shape[0]
    sub = lax.broadcasted_iota(jnp.int32, (8, n), 0)
    lane = lax.broadcasted_iota(jnp.int32, (8, n), 1)
    lane_all = lax.broadcasted_iota(jnp.int32, (n, n), 1)
    for g in range(0, n, 8):
        slab = a[g:g + 8, :]
        cols = [jnp.broadcast_to(slab[:, g + j:g + j + 1], (8, n)) for j in range(8)]
        inside = (lane >= g) & (lane < g + 8)
        slab = jnp.where(inside, jnp.where(lane - g == sub, 1.0, 0.0), slab)
        for k in range(8):
            scale = 1.0 / cols[k][k:k + 1, :]
            row = slab[k:k + 1, :] * scale
            slab = jnp.where(sub == k, row, slab - cols[k] * row)
            for j in range(k + 1, 8):
                crow = cols[j][k:k + 1, :] * scale
                cols[j] = jnp.where(sub == k, crow, cols[j] - cols[k] * crow)
        rest = jnp.where((lane_all >= g) & (lane_all < g + 8), 0.0, a)
        for j in range(8):
            rest = rest - a[:, g + j:g + j + 1] * slab[j:j + 1, :]
        pieces = [slab]
        if g:
            pieces = [rest[:g, :]] + pieces
        if g + 8 < n:
            pieces = pieces + [rest[g + 8:, :]]
        a = jnp.concatenate(pieces, axis=0)
    return a


def dot(a, b, precision=None):
    return jnp.dot(a, b, precision=precision, preferred_element_type=jnp.float32)


def split3(a):
    hi = a.astype(jnp.bfloat16)
    left = a - hi.astype(jnp.float32)
    mid = left.astype(jnp.bfloat16)
    lo = (left - mid.astype(jnp.float32)).astype(jnp.bfloat16)
    return hi, mid, lo


def kernel(n, lower, x_hbm, mask_ref, steer_ref, amf_ref, pow_ref,
           xt, gram, gram_rx, part, rs_rx, red, red_rx, mat, inv, ag_rx, fwd_rx, full,
           lsem, xs, xr, gs, gr, rss, rsr, ds, dr, ags, agr, fs, fr):
    r = lax.axis_index("rng")
    c = lax.axis_index("chn")
    other = 1 - c
    bins, chans, half = xt.shape
    width = chans // 2
    mine = pl.ds(pl.multiple_of(c * width, 8), width)
    nb = chans // T
    share = len(lower) // 2
    rows = share * T

    barrier = pltpu.get_barrier_semaphore()
    pl.semaphore_signal(barrier, inc=1, device_id={"chn": other}, device_id_type=MESH)
    for d in range(1, n):
        pl.semaphore_signal(barrier, inc=1, device_id={"rng": lax.rem(r + d, n)}, device_id_type=MESH)

    order = [lax.rem(r + d, n) for d in range(1, n)] + [r]
    loads = []
    for i, b in enumerate(order):
        cp = pltpu.make_async_copy(x_hbm.at[b, :, pl.ds(pl.multiple_of(c * half, T), half)], xt.at[b, mine, :], lsem.at[i])
        cp.start()
        loads.append(cp)
    pl.semaphore_wait(barrier, n)

    def remote(src, dst, send, recv, where):
        cp = pltpu.make_async_remote_copy(src_ref=src, dst_ref=dst, send_sem=send, recv_sem=recv,
                                          device_id=where, device_id_type=MESH)
        cp.start()
        return cp

    swaps = [remote(x_hbm.at[b, :, pl.ds(pl.multiple_of(other * half, T), half)], xt.at[b, mine, :],
                    xs.at[i], xr.at[i], {"chn": other}) for i, b in enumerate(order)]

    sends = []

    def reduce_pair(i, b):
        swap = gsw[i]
        swap.wait()
        for s in range(share):
            part[b, s * T:(s + 1) * T, :] = gram[b, c * share + s] + gram_rx[b, s]
        count = jnp.sum(mask_ref[pl.ds(b, 1), :].astype(jnp.float32))
        part[b, rows:rows + 8, :] = jnp.full((8, T), count, jnp.float32)
        if i < n - 1:
            sends.append(remote(part.at[b], rs_rx.at[i], rss.at[i], rsr.at[i], {"rng": b}))

    gsw = []
    for i, b in enumerate(order):
        loads[i].wait()
        swaps[i].wait()
        mask = mask_ref[pl.ds(b, 1), pl.ds(pl.multiple_of(c * half, T), half)].astype(jnp.bfloat16)
        xb = xt[b]
        g = lax.dot_general(xb * mask, xb, (((1,), (1,)), ((), ())), preferred_element_type=jnp.float32)
        for s, (p, q) in enumerate(lower):
            gram[b, s] = g[p * T:(p + 1) * T, q * T:(q + 1) * T]
        gsw.append(remote(gram.at[b, pl.ds(other * share, share)], gram_rx.at[b], gs.at[i], gr.at[i], {"chn": other}))
        if i:
            reduce_pair(i - 1, order[i - 1])
    reduce_pair(n - 1, r)

    total = part[r]
    for cp in sends:
        cp.wait()
    for d in range(n - 1):
        total = total + rs_rx[d]
    red[...] = total
    cp = remote(red, red_rx, ds, dr, {"chn": other})
    scale = jnp.maximum(total[rows:rows + 1, :], 1.0)
    cp.wait()
    diag = jnp.where(lax.broadcasted_iota(jnp.int32, (T, T), 0) == lax.broadcasted_iota(jnp.int32, (T, T), 1), LOAD, 0.0)
    for s, (p, q) in enumerate(lower):
        lo = (s % share) * T
        a, b = red[lo:lo + T, :], red_rx[lo:lo + T, :]
        block = jnp.where(c == s // share, a, b) / scale
        if p == q:
            mat[p, p] = block + diag
        else:
            mat[p, q] = block
            mat[q, p] = block.T

    @pl.loop(0, nb)
    def _(p):
        tile = invert_tile(mat[p, p])
        others = [lax.rem(p + d, nb) for d in range(1, nb)]
        cross = [dot(tile, mat[p, j], HIGH) for j in others]
        for i in others:
            col = mat[i, p]
            for j, e in zip(others, cross):
                mat[i, j] = mat[i, j] - dot(col, e, HIGH)
            mat[i, p] = -dot(col, tile, HIGH)
        mat[p, p] = tile
        for j, e in zip(others, cross):
            mat[p, j] = e

    for s, (p, q) in enumerate(lower):
        inv[s] = mat[p, q]
    gathers = [remote(inv.at[pl.ds(c * share, share)], ag_rx.at[d - 1], ags.at[d - 1], agr.at[d - 1],
                      {"rng": lax.rem(r + d, n)}) for d in range(1, n)]
    steer = steer_ref[...]
    k = steer.shape[0]

    def finish(b, blocks):
        for (p, q), block in zip(lower, blocks):
            full[p * T:(p + 1) * T, q * T:(q + 1) * T] = block
            if p != q:
                full[q * T:(q + 1) * T, p * T:(p + 1) * T] = block.T
        s = full[...]
        f = dot(steer, s, HIGH)
        power = jnp.sum(f * steer, axis=1, keepdims=True)
        xb = xt[b]
        y = sum(dot(m, xb) for m in split3(s))
        pow_ref[b] = jnp.sum(y * xb.astype(jnp.float32), axis=0, keepdims=True) / chans
        z = sum(dot(m, xb) for m in split3(f))
        amf_ref[b] = z * z / power

    finish(r, [inv[s] for s in range(len(lower))])
    forwards = []
    for d in range(1, n):
        gathers[d - 1].wait()
        forwards.append(remote(ag_rx.at[d - 1], fwd_rx.at[d - 1], fs.at[d - 1], fr.at[d - 1], {"chn": other}))
    for d in range(1, n):
        forwards[d - 1].wait()
        blocks = [jnp.where(c == s // share, ag_rx[d - 1, s % share], fwd_rx[d - 1, s % share])
                  for s in range(len(lower))]
        finish(lax.rem(r - d + n, n), blocks)


def fused_body(samples, train_mask, angles):
    bins, gates, width = samples.shape
    n = lax.axis_size("rng")
    half, chans = gates // 2, 2 * width
    nb = chans // T
    lower = [(i, j) for i in range(nb) for j in range(i + 1)]
    share = len(lower) // 2
    steer = steering(angles, chans).T
    f32, bf16 = jnp.float32, jnp.bfloat16
    sem = pltpu.SemaphoreType.DMA
    vmem = pl.BlockSpec(memory_space=pltpu.VMEM)
    rows = share * T + 8
    amf, power = pl.pallas_call(
        functools.partial(kernel, n, lower),
        name="amf",
        out_shape=(jax.ShapeDtypeStruct((bins, steer.shape[0], half), f32),
                   jax.ShapeDtypeStruct((bins, 1, half), f32)),
        in_specs=[pl.BlockSpec(memory_space=pl.ANY), vmem, vmem],
        out_specs=(vmem, vmem),
        scratch_shapes=[
            pltpu.VMEM((bins, chans, half), bf16),
            pltpu.VMEM((bins, len(lower), T, T), f32),
            pltpu.VMEM((bins, share, T, T), f32),
            pltpu.VMEM((bins, rows, T), f32),
            pltpu.VMEM((n - 1, rows, T), f32),
            pltpu.VMEM((rows, T), f32),
            pltpu.VMEM((rows, T), f32),
            pltpu.VMEM((nb, nb, T, T), f32),
            pltpu.VMEM((len(lower), T, T), f32),
            pltpu.VMEM((n - 1, share, T, T), f32),
            pltpu.VMEM((n - 1, share, T, T), f32),
            pltpu.VMEM((chans, chans), f32),
            sem((n,)), sem((n,)), sem((n,)), sem((n,)), sem((n,)),
            sem((n - 1,)), sem((n - 1,)), sem, sem,
            sem((n - 1,)), sem((n - 1,)), sem((n - 1,)), sem((n - 1,)),
        ],
        compiler_params=pltpu.CompilerParams(collective_id=0, has_side_effects=True, vmem_limit_bytes=56 * 2**20),
    )(jnp.swapaxes(samples, 1, 2), train_mask, steer)
    return amf, power[:, 0, :]


def solution(mesh):
    placed = (P(("cpi", "bin"), "rng", "chn"), P(("cpi", "bin"), "rng"), P("cpi"))

    def body(samples, train_mask, angles):
        bins, gates, width = samples.shape
        nb = 2 * width // T
        fits = (mesh.shape["chn"] == 2 and mesh.shape["rng"] == bins and bins > 1 and (2 * width) % T == 0
                and gates % (2 * T) == 0 and nb * (nb + 1) // 2 % 2 == 0)
        return (fused_body if fits else plain_body)(samples, train_mask, angles)

    return jax.shard_map(
        body,
        mesh=mesh,
        in_specs=placed,
        out_specs=(P(("cpi", "bin"), None, ("rng", "chn")), P(("cpi", "bin"), ("rng", "chn"))),
        check_vma=False,
    )
```
